128 devices in a mesh: dp: 8 (over x, core), pipe: 4 (over y), tensor: 4 (over z).
Axes of the slice: x: 4, y: 4, z: 4, core: 2. Of those that a mesh axis runs over, the one named last changes fastest.
Arguments:
- support_tokens: int32 [64, 32], P(('dp', 'pipe')), may hold values from 0 to 64127
- support_lengths: int32 [64], P(('dp', 'pipe')), may hold values from 1 to 32
- support_labels: int32 [64, 1], P(('dp', 'pipe')), may hold values from 0 to 31
- query_tokens: int32 [32, 32], P(('dp', 'pipe')), may hold values from 0 to 64127
- query_lengths: int32 [32], P(('dp', 'pipe')), may hold values from 1 to 32
- query_episodes: int32 [32], P(('dp', 'pipe')), may hold values from 0 to 1
- embedding: bfloat16 [64128, 4096], P(('dp', 'pipe'), 'tensor'), may hold values from -18 to 18
- attn_gain: float32 [4, 4096], P('pipe'), may hold values from 0.5 to 1.5
- query_weight: bfloat16 [4, 4096, 4096], P('pipe', None, 'tensor'), may hold values from -1 to 1
- key_weight: bfloat16 [4, 4096, 1024], P('pipe', None, 'tensor'), may hold values from -16 to 16
- value_weight: bfloat16 [4, 4096, 1024], P('pipe', None, 'tensor'), may hold values from -0.09375 to 0.09375
- out_weight: bfloat16 [4, 4096, 4096], P('pipe', 'tensor'), may hold values from -0.09375 to 0.09375
- final_gain: float32 [4096], replicated, may hold values from 0.5 to 1.5
Outputs:
- prototypes: float32 [32, 4096], P(None, 'tensor')
- logits: float32 [32, 16], P(('dp', 'pipe'))
The draws below stay inside these ranges and needn't reach their ends.
Inputs may be any that keep to these rules, and one draw needn't show every extreme that they name: `support_labels`: every class is the label of at least one support sequence.
All inputs are finite; a program needn't handle non-finite values.
Results may differ from the reference program's by a relative error of at most 0.024.
Values may be sent and summed in bfloat16 or wider, within the bound.
A program may use at most 128 MiB of HBM per device.

```python
import math
import jax
import jax.numpy as jnp
import numpy as np
from jax import lax

D = 4096
HEADS = 32
KV_HEADS = 8
HEAD_DIM = 128
VOCAB = 64128
WAYS = 16
EPISODES = 2
LEN = 32
LAYERS = 4
SUPPORTS = 64
QUERIES = 32
CLASSES = 32
N_TENSOR = 4


def shared_projection(key):
    base = jax.random.normal(jax.random.fold_in(key, 7), (LAYERS, D, HEADS * HEAD_DIM), jnp.float32)
    return jnp.clip(base, -6.0, 6.0) / math.sqrt(D)


def draw_query_weight(key, part):
    return shared_projection(key).astype(jnp.bfloat16)


def draw_key_weight(key, part):
    noise = jax.random.normal(jax.random.fold_in(key, 13), (LAYERS, D, KV_HEADS * HEAD_DIM), jnp.float32)
    noise = jnp.clip(noise, -6.0, 6.0) / math.sqrt(D)
    return noise.astype(jnp.bfloat16)


def draw_embedding(key, part):
    row_scale = jnp.exp(jax.random.uniform(jax.random.fold_in(key, 21), (VOCAB, 1), jnp.float32, math.log(0.3), math.log(3.0)))
    values = jnp.clip(jax.random.normal(jax.random.fold_in(key, 27), (VOCAB, D), jnp.float32), -6.0, 6.0)
    return (values * row_scale).astype(jnp.bfloat16)


def place_ends(entries, rng, low, high):
    extent = entries.shape
    index_at = [jax.random.randint(jax.random.fold_in(rng, axis), (), 0, extent[axis]) for axis in range(len(extent))]
    entries = entries.at[tuple(index_at)].set(low)
    longest = extent.index(max(extent))
    index_at[longest] = (index_at[longest] + 1) % extent[longest]
    return entries.at[tuple(index_at)].set(high)


def steps_of(rng, dims, pieces, least, top_value):
    gain = 1.0
    for axis_at, blocks in pieces:
        steps = jax.random.uniform(jax.random.fold_in(jax.random.fold_in(rng, 6), axis_at), (blocks,), jnp.float32, least / len(pieces), top_value / len(pieces))
        gain = gain * jnp.repeat(jnp.exp(steps), dims[axis_at] // blocks).reshape((-1,) + (1,) * (len(dims) - 1 - axis_at))
    return gain


def cumulative_ranks(number_of, lean):
    portions = [(1 << 20) // math.isqrt(rank ** lean) + 1 for rank in range(1, number_of + 1)]
    spread = 1 + sum(portions) // (1 << 30)
    return np.cumsum(np.array([max(1, weight // spread) for weight in portions]))


def ranked_ids(rng, dims, number_of, slope):
    table = cumulative_ranks(number_of, slope)
    pick = jax.random.randint(jax.random.fold_in(rng, 1), dims, 0, int(table[number_of - 1]))
    standing = jnp.searchsorted(jnp.asarray(table, jnp.int32), pick, side="right")
    return jax.random.permutation(jax.random.fold_in(rng, 2), number_of)[standing].astype(jnp.int32)


def picks_of(rng, rows, amount, top, lift):
    ranking = jax.random.permutation(jax.random.fold_in(rng, 1), amount)
    favour = ranking
    for power in range(3):
        favour = favour * favour // amount
    favour = favour * lift // amount
    lots = jax.random.randint(jax.random.fold_in(rng, 2), (rows, amount), 0, 4096) + favour
    holders = jax.random.permutation(jax.random.fold_in(rng, 3), rows)[jnp.arange(amount) % rows]
    lots = jnp.where(jnp.arange(rows)[:, None] == holders[None, :], 1 << 14, lots)
    score = lots * amount + jnp.arange(amount)
    return lax.top_k(score.astype(jnp.int32), top)[1].astype(jnp.int32)


def gaussian(own_key, extent, scale, most, cuts=(), held_as=jnp.bfloat16):
    values = scale * jax.random.normal(own_key, extent, jnp.float32)
    if cuts:
        values = values * steps_of(own_key, extent, cuts, -0.22, 0.18)
    return jnp.clip(values, -most, most).astype(held_as)


def setup_inputs(seed: int = 0) -> dict:
    key_of = jax.random.split(jax.random.key(seed), 14)
    support_tokens = place_ends(ranked_ids(key_of[0], (SUPPORTS, LEN), VOCAB, 2), jax.random.fold_in(key_of[0], 3), 0, VOCAB - 1).astype(jnp.int32)
    support_lengths = place_ends(jax.random.randint(key_of[1], (SUPPORTS,), 1, LEN + 1), jax.random.fold_in(key_of[1], 1), 1, LEN).astype(jnp.int32)
    support_labels = picks_of(key_of[2], SUPPORTS, CLASSES, 1, 0)
    query_tokens = place_ends(ranked_ids(key_of[3], (QUERIES, LEN), VOCAB, 2), jax.random.fold_in(key_of[3], 3), 0, VOCAB - 1).astype(jnp.int32)
    query_lengths = place_ends(jax.random.randint(key_of[4], (QUERIES,), 1, LEN + 1), jax.random.fold_in(key_of[4], 1), 1, LEN).astype(jnp.int32)
    query_episodes = place_ends(jax.random.randint(key_of[5], (QUERIES,), 0, EPISODES), jax.random.fold_in(key_of[5], 1), 0, EPISODES - 1).astype(jnp.int32)
    embedding = draw_embedding(jax.random.fold_in(key_of[13], 71), 0)
    attn_gain = jnp.clip(1.0 + 0.1 * jax.random.normal(key_of[7], (LAYERS, D), jnp.float32), 0.5, 1.5)
    query_weight = draw_query_weight(jax.random.fold_in(key_of[13], 71), 0)
    key_weight = draw_key_weight(jax.random.fold_in(key_of[13], 71), 0)
    value_weight = gaussian(key_of[10], (LAYERS, D, KV_HEADS * HEAD_DIM), D ** -0.5, 0.09375, ((0, 4), (2, 4)))
    out_weight = gaussian(key_of[11], (LAYERS, HEADS * HEAD_DIM, D), (HEADS * HEAD_DIM) ** -0.5, 0.09375, ((0, 4), (1, 4)))
    final_gain = jnp.clip(1.0 + 0.1 * jax.random.normal(key_of[12], (D,), jnp.float32), 0.5, 1.5)
    return {"support_tokens": support_tokens, "support_lengths": support_lengths, "support_labels": support_labels, "query_tokens": query_tokens, "query_lengths": query_lengths, "query_episodes": query_episodes, "embedding": embedding, "attn_gain": attn_gain, "query_weight": query_weight, "key_weight": key_weight, "value_weight": value_weight, "out_weight": out_weight, "final_gain": final_gain}


epsilon = 1e-05
rotary_base = 500000.0

def normed_values(hidden, gain_vector):
    values = hidden.astype(jnp.float32)
    mean_square = lax.optimization_barrier(jnp.mean(values * values, axis=-1, keepdims=True))
    return values * lax.rsqrt(mean_square + epsilon) * gain_vector.astype(jnp.float32)

def rotate(heads_in, seq_len):
    half_dim = HEAD_DIM // 2
    freqs = jnp.exp(-math.log(rotary_base) * jnp.arange(half_dim, dtype=jnp.float32) * (2.0 / HEAD_DIM))
    angles = jnp.arange(seq_len, dtype=jnp.float32)[:, None] * freqs[None, :]
    cosine = jnp.cos(angles)[None, :, None, :]
    sine = jnp.sin(angles)[None, :, None, :]
    first_half = heads_in[..., :half_dim]
    second_half = heads_in[..., half_dim:]
    return jnp.concatenate([first_half * cosine - second_half * sine, second_half * cosine + first_half * sine], axis=-1)

def attention_block(hidden, gain_vector, query_proj, key_proj, value_proj, out_proj, seq_lengths):
    seq_count, seq_len, width = hidden.shape
    normed = normed_values(hidden, gain_vector).astype(jnp.bfloat16).reshape(seq_count * seq_len, width)
    query_heads = jnp.dot(normed, query_proj, preferred_element_type=jnp.float32).reshape(seq_count, seq_len, HEADS, HEAD_DIM)
    key_heads = jnp.dot(normed, key_proj, preferred_element_type=jnp.float32).reshape(seq_count, seq_len, KV_HEADS, HEAD_DIM)
    value_heads = jnp.dot(normed, value_proj, preferred_element_type=jnp.float32).reshape(seq_count, seq_len, KV_HEADS, HEAD_DIM)
    query_heads = rotate(query_heads, seq_len).astype(jnp.bfloat16)
    key_heads = rotate(key_heads, seq_len).astype(jnp.bfloat16)
    value_heads = value_heads.astype(jnp.bfloat16)
    group_size = HEADS // KV_HEADS
    grouped = query_heads.astype(jnp.float32).reshape(seq_count, seq_len, KV_HEADS, group_size, HEAD_DIM)
    scores = jnp.einsum('sikgd,sjkd->skgij', grouped, key_heads.astype(jnp.float32)) / math.sqrt(HEAD_DIM)
    positions = jnp.arange(seq_len)
    causal = positions[None, :] <= positions[:, None]
    visible = causal[None, :, :] & (positions[None, None, :] < seq_lengths[:, None, None])
    scores = jnp.where(visible[:, None, None, :, :], scores, -1e+30)
    weights = jax.nn.softmax(scores, axis=-1).astype(jnp.bfloat16)
    mixed = jnp.einsum('skgij,sjkd->sikgd', weights.astype(jnp.float32), value_heads.astype(jnp.float32))
    mixed = mixed.astype(jnp.bfloat16).reshape(seq_count * seq_len, HEADS * HEAD_DIM)
    shard_width = HEADS * HEAD_DIM // N_TENSOR
    running = jnp.zeros((seq_count * seq_len, width), jnp.float32)
    for shard_index in range(N_TENSOR):
        low = shard_index * shard_width
        term = jnp.dot(mixed[:, low:low + shard_width], out_proj[low:low + shard_width], preferred_element_type=jnp.float32)
        running = running + lax.optimization_barrier(term.astype(jnp.bfloat16)).astype(jnp.float32)
    updated = hidden.astype(jnp.float32).reshape(seq_count * seq_len, width) + running
    return updated.astype(jnp.bfloat16).reshape(seq_count, seq_len, width)

def reference(support_tokens, support_lengths, support_labels, query_tokens, query_lengths, query_episodes, embedding, attn_gain, query_weight, key_weight, value_weight, out_weight, final_gain):
    token_ids = jnp.concatenate([support_tokens, query_tokens], axis=0)
    seq_lengths = jnp.concatenate([support_lengths, query_lengths], axis=0)
    hidden = jnp.take(embedding, token_ids, axis=0)
    for layer_index in range(LAYERS):
        hidden = attention_block(hidden, attn_gain[layer_index], query_weight[layer_index], key_weight[layer_index], value_weight[layer_index], out_weight[layer_index], seq_lengths)
    final = normed_values(hidden, final_gain)
    live = (jnp.arange(LEN)[None, :] < seq_lengths[:, None]).astype(jnp.float32)
    pooled = lax.optimization_barrier(jnp.sum(final * live[:, :, None], axis=1)) / seq_lengths[:, None].astype(jnp.float32)
    support_pooled = pooled[:SUPPORTS]
    query_pooled = pooled[SUPPORTS:]
    onehot = (support_labels[:, 0][:, None] == jnp.arange(CLASSES)[None, :]).astype(jnp.float32)
    class_total = jnp.dot(onehot.T, support_pooled, precision=lax.Precision.HIGHEST)
    class_count = lax.optimization_barrier(jnp.sum(onehot, axis=0))
    prototypes = class_total / class_count[:, None]
    chosen = prototypes.reshape(EPISODES, WAYS, D)[query_episodes]
    distance = lax.optimization_barrier(jnp.sum((query_pooled[:, None, :] - chosen) ** 2, axis=-1))
    logits = -distance / math.sqrt(D)
    return (prototypes, logits)
```

```python
import functools
import math

import jax
import jax.numpy as jnp
from jax import lax
from jax.experimental import pallas as pl
from jax.experimental.pallas import tpu as pltpu
from jax.sharding import PartitionSpec as P

D = 4096
HEAD_DIM = 128
WAYS = 16
EPISODES = 2


epsilon = 1e-05
rotary_base = 500000.0


def in_order(blocks, dim):
    blocks = jnp.moveaxis(blocks, 0, dim)
    dims = blocks.shape
    return blocks.reshape(*dims[:dim], dims[dim] * dims[dim + 1], *dims[dim + 2 :])


def sent_to_all(shard, axis):
    copies = jnp.broadcast_to(shard, (lax.axis_size(axis), *shard.shape))
    return lax.all_to_all(copies, axis, split_axis=0, concat_axis=0, tiled=True)


def collect(shard, axis, dim):
    return in_order(sent_to_all(shard, axis), dim)


def split_up(shard, dim, length):
    dims = shard.shape
    blocks = shard.reshape(*dims[:dim], length, dims[dim] // length, *dims[dim + 1 :])
    return jnp.moveaxis(blocks, dim, 0)


def sum_at_owner(shard, axis, dim):
    length = lax.axis_size(axis)
    blocks = lax.all_to_all(split_up(shard, dim, length), axis, 0, 0, tiled=True)
    return jnp.sum(blocks.astype(jnp.float32), axis=0)


def passed_along(block, axis, distance):
    devices = range(lax.axis_size(axis))
    route = [((i - distance) % len(devices), i) for i in devices]
    return lax.ppermute(block, axis, route)


def over_copies(shard, axis):
    return sent_to_all(shard, axis).astype(jnp.float32).sum(axis=0)


def rotate(heads_in, seq_len):
    half_dim = HEAD_DIM // 2
    freqs = jnp.exp(
        -math.log(rotary_base) * jnp.arange(half_dim, dtype=jnp.float32) * (2.0 / HEAD_DIM)
    )
    angles = jnp.arange(seq_len, dtype=jnp.float32)[:, None] * freqs[None, :]
    cosine = jnp.cos(angles)[None, :, None, :]
    sine = jnp.sin(angles)[None, :, None, :]
    first_half = heads_in[..., :half_dim]
    second_half = heads_in[..., half_dim:]
    return jnp.concatenate(
        [first_half * cosine - second_half * sine, second_half * cosine + first_half * sine],
        axis=-1,
    )


def whole_rows(hidden):
    return collect(hidden, "tensor", 1)


def whole_values(full_rows, gain_vector):
    values = full_rows.astype(jnp.float32)
    mean_square = jnp.mean(values * values, axis=-1, keepdims=True)
    return values * lax.rsqrt(mean_square + epsilon) * gain_vector


def plain_shards(
    support_tokens,
    support_lengths,
    support_labels,
    query_tokens,
    query_lengths,
    query_episodes,
    embedding,
    attn_gain,
    query_weight,
    key_weight,
    value_weight,
    out_weight,
    final_gain,
):
    group_count = lax.axis_size(("dp", "pipe"))
    sections = lax.axis_size("pipe")
    sup_dev, seq_len = support_tokens.shape
    qry_dev = query_tokens.shape[0]
    seq_count = sup_dev + qry_dev
    row_count = seq_count * seq_len
    table_rows, width = embedding.shape
    column_start = lax.axis_index("tensor") * width
    all_support, all_query, every_sup_len, every_qry_len = (
        lax.all_gather(support_tokens, ("dp", "pipe"), axis=0, tiled=True),
        lax.all_gather(query_tokens, ("dp", "pipe"), axis=0, tiled=True),
        lax.all_gather(support_lengths, ("dp", "pipe"), axis=0, tiled=True),
        lax.all_gather(query_lengths, ("dp", "pipe"), axis=0, tiled=True),
    )
    token_flat = jnp.concatenate(
        [all_support.reshape(group_count, sup_dev * seq_len), all_query], axis=1
    ).reshape(group_count * row_count)
    local_ids = token_flat - lax.axis_index(("dp", "pipe")) * table_rows
    inside = (local_ids >= 0) & (local_ids < table_rows)
    picked = jnp.take(embedding, jnp.clip(local_ids, 0, table_rows - 1), axis=0)
    picked = jnp.where(inside[:, None], picked, jnp.zeros_like(picked))
    replies = lax.all_to_all(picked, ("dp", "pipe"), split_axis=0, concat_axis=0, tiled=True)
    hidden = jnp.sum(
        replies.reshape(group_count, row_count, width).astype(jnp.float32), axis=0
    ).astype(jnp.bfloat16)
    seq_lengths = jnp.concatenate([support_lengths, query_lengths], axis=0)
    query_proj = query_weight[0]
    key_proj = key_weight[0]
    value_proj = value_weight[0]
    out_proj = out_weight[0]
    gain_vector = attn_gain[0]
    local_heads = query_proj.shape[1] // HEAD_DIM
    local_groups = key_proj.shape[1] // HEAD_DIM
    group_size = local_heads // local_groups
    w_in = jnp.concatenate([query_proj, key_proj, value_proj], axis=1)
    query_cols = local_heads * HEAD_DIM
    key_cols = local_groups * HEAD_DIM
    positions = jnp.arange(seq_len)
    causal = positions[None, :] <= positions[:, None]

    def section_block(stream, lengths_here):
        normed = whole_values(whole_rows(stream), gain_vector).astype(jnp.bfloat16)
        projected = jnp.dot(normed, w_in, preferred_element_type=jnp.float32)
        query_heads = projected[:, :query_cols].reshape(seq_count, seq_len, local_heads, HEAD_DIM)
        key_heads = projected[:, query_cols : query_cols + key_cols].reshape(
            seq_count, seq_len, local_groups, HEAD_DIM
        )
        value_heads = (
            projected[:, query_cols + key_cols :]
            .reshape(seq_count, seq_len, local_groups, HEAD_DIM)
            .astype(jnp.bfloat16)
        )
        query_heads = (
            rotate(query_heads, seq_len)
            .astype(jnp.bfloat16)
            .reshape(seq_count, seq_len, local_groups, group_size, HEAD_DIM)
        )
        key_heads = rotate(key_heads, seq_len).astype(jnp.bfloat16)
        scores = jnp.einsum(
            "sikgd,sjkd->skgij", query_heads, key_heads, preferred_element_type=jnp.float32
        ) / math.sqrt(HEAD_DIM)
        visible = causal[None, :, :] & (positions[None, None, :] < lengths_here[:, None, None])
        scores = jnp.where(visible[:, None, None, :, :], scores, -1e30)
        weights = jax.nn.softmax(scores, axis=-1).astype(jnp.bfloat16)
        mixed = jnp.einsum(
            "skgij,sjkd->sikgd", weights, value_heads, preferred_element_type=jnp.float32
        )
        mixed = mixed.astype(jnp.bfloat16).reshape(row_count, query_cols)
        partial_out = jnp.dot(mixed, out_proj, preferred_element_type=jnp.float32)
        summed = sum_at_owner(partial_out.astype(jnp.bfloat16), "tensor", 1)
        return (stream.astype(jnp.float32) + summed).astype(jnp.bfloat16)

    section_index = lax.axis_index("pipe")
    dp_base = lax.axis_index("dp") * sections

    def tick(tick_index, stream):
        held_group = dp_base + (section_index - tick_index) % sections
        sup_part = lax.dynamic_slice_in_dim(every_sup_len, held_group * sup_dev, sup_dev)
        qry_part = lax.dynamic_slice_in_dim(every_qry_len, held_group * qry_dev, qry_dev)
        lengths_here = jnp.concatenate([sup_part, qry_part], axis=0)
        first_tick = (tick_index - section_index) % sections
        active = (first_tick <= tick_index) & (tick_index < first_tick + sections)
        computed = section_block(stream, lengths_here)
        stream = jnp.where(active, computed, stream)
        return passed_along(stream, "pipe", 1)

    hidden = lax.fori_loop(0, 2 * sections, tick, hidden)
    final = lax.dynamic_slice_in_dim(
        whole_values(whole_rows(hidden), final_gain), column_start, width, 1
    )
    live = (positions[None, :] < seq_lengths[:, None]).astype(jnp.float32)
    pooled = jnp.sum(
        final.reshape(seq_count, seq_len, width) * live[:, :, None], axis=1
    ) / seq_lengths[:, None].astype(jnp.float32)
    support_pooled = pooled[:sup_dev]
    query_pooled = pooled[sup_dev:]
    class_count_all = EPISODES * WAYS
    onehot = (support_labels[:, 0][:, None] == jnp.arange(class_count_all)[None, :]).astype(
        jnp.float32
    )
    class_total = jnp.dot(onehot.T, support_pooled, precision=lax.Precision.HIGHEST)
    class_count = jnp.sum(onehot, axis=0)
    class_total, class_count = (
        over_copies(class_total.astype(jnp.bfloat16), ("dp", "pipe")).astype(jnp.float32),
        over_copies(class_count.astype(jnp.bfloat16), ("dp", "pipe")).astype(jnp.float32),
    )
    prototypes = class_total / class_count[:, None]
    episode_pick = (query_episodes[:, None] == jnp.arange(EPISODES)[None, :]).astype(jnp.float32)
    chosen = jnp.einsum(
        "qe,ewc->qwc",
        episode_pick,
        prototypes.reshape(EPISODES, WAYS, width),
        precision=lax.Precision.HIGHEST,
    )
    partial_distance = jnp.sum((query_pooled[:, None, :] - chosen) ** 2, axis=-1)
    distance = lax.psum(partial_distance, "tensor")
    logits = -distance / math.sqrt(D)
    return (prototypes, logits)


MESH = pl.DeviceIdType.MESH
GROUPS = 32
PIPE = 4
TENSOR = 4
LANES = 8
STEPS = 4
SLOTS = 64
CAP = 16
SHARD = 1024
HIGH = lax.Precision.HIGHEST


def place():
    return lax.axis_index("dp"), lax.axis_index("pipe"), lax.axis_index("tensor")


def peer(dp, pipe, tensor):
    return {"dp": dp, "pipe": pipe, "tensor": tensor}


def greet(with_tensor):
    dp, pipe, tensor = place()
    mine = dp * PIPE + pipe
    barrier = pltpu.get_barrier_semaphore()
    for step in range(1, GROUPS):
        other = lax.rem(mine + step, GROUPS)
        pl.semaphore_signal(
            barrier,
            inc=1,
            device_id=peer(other // PIPE, lax.rem(other, PIPE), tensor),
            device_id_type=MESH,
        )
    count = GROUPS - 1
    if with_tensor:
        for step in range(1, TENSOR):
            pl.semaphore_signal(
                barrier,
                inc=1,
                device_id=peer(dp, pipe, lax.rem(tensor + step, TENSOR)),
                device_id_type=MESH,
            )
        count += TENSOR - 1
    pl.semaphore_wait(barrier, count)


def remote(src, dst, send_sem, recv_sem, device):
    return pltpu.make_async_remote_copy(
        src_ref=src,
        dst_ref=dst,
        send_sem=send_sem,
        recv_sem=recv_sem,
        device_id=device,
        device_id_type=MESH,
    )


def ids_kernel(row_ref, out_ref, held, send_sem, recv_sem):
    dp, pipe, tensor = place()
    mine = dp * PIPE + pipe
    greet(False)
    copies = []
    for step in range(1, GROUPS):
        other = lax.rem(mine + step, GROUPS)
        copy = remote(
            row_ref,
            held.at[mine],
            send_sem.at[step],
            recv_sem.at[step],
            peer(other // PIPE, lax.rem(other, PIPE), tensor),
        )
        copy.start()
        copies.append(copy)
    held[mine] = row_ref[...]
    for step in range(1, GROUPS):
        source = lax.rem(mine - step + GROUPS, GROUPS)
        remote(
            row_ref, held.at[source], send_sem.at[step], recv_sem.at[step], peer(dp, pipe, tensor)
        ).wait_recv()
    out_ref[...] = held[...]
    for copy in copies:
        copy.wait_send()


def share_ids(row):
    return pl.pallas_call(
        ids_kernel,
        out_shape=jax.ShapeDtypeStruct((GROUPS, 1, 128), jnp.int32),
        in_specs=[pl.BlockSpec(memory_space=pltpu.VMEM)],
        out_specs=pl.BlockSpec(memory_space=pltpu.VMEM),
        scratch_shapes=[
            pltpu.VMEM((GROUPS, 1, 128), jnp.int32),
            pltpu.SemaphoreType.DMA((GROUPS,)),
            pltpu.SemaphoreType.DMA((GROUPS,)),
        ],
        compiler_params=pltpu.CompilerParams(collective_id=0, has_side_effects=True),
        name="share_ids",
    )(row).reshape(GROUPS, 128)


def trunk_kernel(
    rows_ref,
    slot_ref,
    cos_ref,
    sin_ref,
    bias_ref,
    gain_ref,
    wq_ref,
    wk_ref,
    wv_ref,
    wo_ref,
    out_ref,
    w_in,
    w_out,
    emb,
    ag,
    rs,
    po,
    moved,
    nbuf,
    mix,
    w_sem,
    emb_send,
    emb_recv,
    ag_send,
    ag_recv,
    rs_send,
    rs_recv,
    mv_send,
    mv_recv,
):
    dp, pipe, tensor = place()
    mine = dp * PIPE + pipe
    loads = [
        pltpu.make_async_copy(wq_ref.at[0], w_in.at[:, pl.ds(0, 1024)], w_sem.at[0]),
        pltpu.make_async_copy(wk_ref.at[0], w_in.at[:, pl.ds(1024, 256)], w_sem.at[1]),
        pltpu.make_async_copy(wv_ref.at[0], w_in.at[:, pl.ds(1280, 256)], w_sem.at[2]),
    ] + [
        pltpu.make_async_copy(
            wo_ref.at[0, :, pl.ds(i * SHARD, SHARD)], w_out.at[i], w_sem.at[3 + i]
        )
        for i in range(TENSOR)
    ]
    for load in loads:
        load.start()
    greet(True)

    def emb_copy(lane):
        return remote(
            rows_ref.at[lane],
            emb.at[mine],
            emb_send.at[lane],
            emb_recv.at[mine],
            peer(lane, 0, tensor),
        )

    for lane in range(LANES):

        @pl.when(mine != lane * PIPE)
        def _():
            emb_copy(lane).start()

    @pl.when(pipe == 0)
    def _():
        emb[mine] = rows_ref[dp]

        def wait_source(source, carry):
            @pl.when(source != mine)
            def _():
                remote(
                    rows_ref.at[0],
                    emb.at[source],
                    emb_send.at[0],
                    emb_recv.at[source],
                    peer(dp, pipe, tensor),
                ).wait_recv()

            return carry

        lax.fori_loop(0, GROUPS, wait_source, 0)

    for load in loads:
        load.wait()

    def ag_copy(step, j):
        other = lax.rem(tensor + j, TENSOR)
        return remote(
            ag.at[step, tensor],
            ag.at[step, tensor],
            ag_send.at[step, j],
            ag_recv.at[step, j],
            peer(dp, pipe, other),
        )

    def rs_copy(step, j):
        other = lax.rem(tensor + j, TENSOR)
        return remote(
            po.at[step, other],
            rs.at[step, tensor],
            rs_send.at[step, j],
            rs_recv.at[step, j],
            peer(dp, pipe, other),
        )

    def mv_copy(step):
        return remote(
            moved.at[step],
            ag.at[step, tensor],
            mv_send.at[step],
            mv_recv.at[step],
            peer(dp, lax.rem(pipe + 1, PIPE), tensor),
        )

    def take(step):
        @pl.when(pipe == 0)
        def _():
            pick = lax.broadcasted_iota(jnp.int32, (SLOTS, GROUPS * CAP), 1)
            onehot = (pick == slot_ref[step]).astype(jnp.float32).astype(jnp.bfloat16)
            table = emb[...].reshape(GROUPS * CAP, SHARD)
            ag[step, tensor] = jnp.dot(
                onehot, table, preferred_element_type=jnp.float32
            ).astype(jnp.bfloat16)

        @pl.when(pipe > 0)
        def _():
            mv_copy(step).wait_recv()

        for j in (2, 1, 3):
            ag_copy(step, j).start()

    def compute(step):
        for j in (1, 3, 2):
            source = lax.rem(tensor - j + TENSOR, TENSOR)
            remote(
                ag.at[step, source],
                ag.at[step, source],
                ag_send.at[step, j],
                ag_recv.at[step, j],
                peer(dp, pipe, tensor),
            ).wait_recv()
        total = jnp.zeros((SLOTS, 1), jnp.float32)
        for s in range(TENSOR):
            values = ag[step, s].astype(jnp.float32)
            total += jnp.sum(values * values, axis=-1, keepdims=True)
        factor = lax.rsqrt(total / D + epsilon)
        for s in range(TENSOR):
            values = ag[step, s].astype(jnp.float32)
            cols = slice(s * SHARD, (s + 1) * SHARD)
            nbuf[:, cols] = (values * factor * gain_ref[:, cols]).astype(jnp.bfloat16)
        cosine = cos_ref[step]
        sine = sin_ref[step]
        bias = bias_ref[step]
        bias4 = jnp.concatenate([bias] * 4, axis=0)
        scale = 1.0 / math.sqrt(HEAD_DIM)

        def turned(block):
            return (block * cosine + pltpu.roll(block, 64, 1) * sine).astype(jnp.bfloat16)

        normed = nbuf[...]
        kv = jnp.dot(normed, w_in[:, 1024:1536], preferred_element_type=jnp.float32)
        for g in range(2):
            qs = jnp.dot(
                normed, w_in[:, g * 512 : (g + 1) * 512], preferred_element_type=jnp.float32
            )
            key = turned(kv[:, g * 128 : (g + 1) * 128])
            value = kv[:, 256 + g * 128 : 256 + (g + 1) * 128].astype(jnp.bfloat16)
            query = jnp.concatenate(
                [turned(qs[:, h * 128 : (h + 1) * 128]) for h in range(4)], axis=0
            )
            scores = lax.dot_general(
                query, key, (((1,), (1,)), ((), ())), preferred_element_type=jnp.float32
            )
            scores = scores * scale + bias4
            top = jnp.max(scores, axis=-1, keepdims=True)
            raised = jnp.exp(scores - top)
            weights = (raised / jnp.sum(raised, axis=-1, keepdims=True)).astype(jnp.bfloat16)
            mixed = jnp.dot(weights, value, preferred_element_type=jnp.float32)
            mixed = mixed.astype(jnp.bfloat16)
            for h in range(4):
                cols = slice(g * 512 + h * 128, g * 512 + (h + 1) * 128)
                mix[:, cols] = mixed[h * SLOTS : (h + 1) * SLOTS]
        for j in (2, 1, 3, 0):
            other = lax.rem(tensor + j, TENSOR)
            part = jnp.dot(mix[...], w_out[other], preferred_element_type=jnp.float32)
            po[step, other] = part.astype(jnp.bfloat16)
            if j:
                rs_copy(step, j).start()

    def settle(step):
        total = po[step, tensor].astype(jnp.float32)
        for j in (1, 3, 2):
            source = lax.rem(tensor - j + TENSOR, TENSOR)
            remote(
                po.at[step, 0],
                rs.at[step, source],
                rs_send.at[step, j],
                rs_recv.at[step, j],
                peer(dp, pipe, tensor),
            ).wait_recv()
            total += rs[step, source].astype(jnp.float32)
        moved[step] = (ag[step, tensor].astype(jnp.float32) + total).astype(jnp.bfloat16)

        @pl.when(pipe < PIPE - 1)
        def _():
            mv_copy(step).start()

    take(0)

    def body(step, carry):
        compute(step)

        @pl.when(step < STEPS - 1)
        def _():
            take(lax.min(step + 1, STEPS - 1))

        settle(step)
        return carry

    lax.fori_loop(0, STEPS, body, 0)
    out_ref[...] = moved[...]

    def drain(step, carry):
        for j in (1, 2, 3):
            ag_copy(step, j).wait_send()
            rs_copy(step, j).wait_send()

        @pl.when(pipe < PIPE - 1)
        def _():
            mv_copy(step).wait_send()

        return carry

    lax.fori_loop(0, STEPS, drain, 0)
    for lane in range(LANES):

        @pl.when(mine != lane * PIPE)
        def _():
            emb_copy(lane).wait_send()


def trunk(rows, slots, cosine, sine, bias, gain, wq, wk, wv, wo):
    vmem = pl.BlockSpec(memory_space=pltpu.VMEM)
    hbm = pl.BlockSpec(memory_space=pl.ANY)
    sems = pltpu.SemaphoreType.DMA
    return pl.pallas_call(
        trunk_kernel,
        out_shape=jax.ShapeDtypeStruct((STEPS, SLOTS, SHARD), jnp.bfloat16),
        in_specs=[vmem] * 6 + [hbm] * 4,
        out_specs=vmem,
        scratch_shapes=[
            pltpu.VMEM((D, 1536), jnp.bfloat16),
            pltpu.VMEM((TENSOR, SHARD, SHARD), jnp.bfloat16),
            pltpu.VMEM((GROUPS, CAP, SHARD), jnp.bfloat16),
            pltpu.VMEM((STEPS, TENSOR, SLOTS, SHARD), jnp.bfloat16),
            pltpu.VMEM((STEPS, TENSOR, SLOTS, SHARD), jnp.bfloat16),
            pltpu.VMEM((STEPS, TENSOR, SLOTS, SHARD), jnp.bfloat16),
            pltpu.VMEM((STEPS, SLOTS, SHARD), jnp.bfloat16),
            pltpu.VMEM((SLOTS, D), jnp.bfloat16),
            pltpu.VMEM((SLOTS, SHARD), jnp.bfloat16),
            sems((7,)),
            sems((LANES,)),
            sems((GROUPS,)),
            sems((STEPS, TENSOR)),
            sems((STEPS, TENSOR)),
            sems((STEPS, TENSOR)),
            sems((STEPS, TENSOR)),
            sems((STEPS,)),
            sems((STEPS,)),
        ],
        compiler_params=pltpu.CompilerParams(
            collective_id=1, has_side_effects=True, vmem_limit_bytes=52 * 1024 * 1024
        ),
        name="trunk",
    )(rows, slots, cosine, sine, bias, gain, wq, wk, wv, wo)


def close_kernel(
    hid_ref,
    weight_ref,
    gain_ref,
    count_ref,
    episode_ref,
    proto_ref,
    logit_ref,
    part,
    parts,
    sq,
    sqs,
    done,
    dones,
    dist,
    dists,
    sq_send,
    sq_recv,
    part_send,
    part_recv,
    done_send,
    done_recv,
    dist_send,
    dist_recv,
):
    dp, pipe, tensor = place()
    mine = dp * PIPE + pipe
    last = PIPE - 1
    tokens = STEPS * SLOTS
    greet(True)

    def sq_copy(j):
        other = lax.rem(tensor + j, TENSOR)
        return remote(sq, sqs.at[j], sq_send.at[j], sq_recv.at[j], peer(dp, pipe, other))

    def part_copy(j):
        other = lax.rem(dp + j, LANES)
        return remote(
            part.at[other], parts.at[j], part_send.at[j], part_recv.at[j], peer(other, pipe, tensor)
        )

    def done_copy(step):
        other = lax.rem(mine + step, GROUPS)
        return remote(
            done,
            dones.at[dp],
            done_send.at[step],
            done_recv.at[dp],
            peer(other // PIPE, lax.rem(other, PIPE), tensor),
        )

    def dist_copy(j):
        other = lax.rem(tensor + j, TENSOR)
        return remote(
            dist, dists.at[j], dist_send.at[j], dist_recv.at[j], peer(dp, pipe, other)
        )

    @pl.when(pipe == last)
    def _():
        values = hid_ref[...].astype(jnp.float32).reshape(tokens, SHARD)
        ones = jnp.ones((8, SHARD), jnp.float32)
        sq[...] = lax.dot_general(
            ones,
            values * values,
            (((1,), (1,)), ((), ())),
            precision=HIGH,
            preferred_element_type=jnp.float32,
        )
        for j in (2, 1, 3):
            sq_copy(j).start()
        total = sq[...]
        for j in (1, 3, 2):
            sq_copy(j).wait_recv()
            total += sqs[j]
        factor = lax.rsqrt(total[0:1] / D + epsilon)
        pooled = jnp.dot(
            weight_ref[...] * factor, values, precision=HIGH, preferred_element_type=jnp.float32
        )
        part[...] = (pooled * gain_ref[...]).reshape(LANES, 8, SHARD)
        for j in range(1, LANES):
            part_copy(j).start()
        whole = part[dp]
        for j in range(1, LANES):
            part_copy(j).wait_recv()
            whole += parts[j]
        done[...] = whole / count_ref[...]
        for step in range(1, GROUPS):
            done_copy(step).start()
        dones[dp] = done[...]

    for lane in range(LANES):

        @pl.when(mine != lane * PIPE + last)
        def _():
            remote(
                done, dones.at[lane], done_send.at[0], done_recv.at[lane], peer(dp, pipe, tensor)
            ).wait_recv()

    for lane in range(LANES):
        proto_ref[lane * 4 : (lane + 1) * 4, :] = dones[lane, 0:4, :]
    query = dones[dp, pl.ds(4 + pipe, 1), :]
    gap = proto_ref[...] - query
    dist[...] = lax.dot_general(
        jnp.ones((8, SHARD), jnp.float32),
        gap * gap,
        (((1,), (1,)), ((), ())),
        precision=HIGH,
        preferred_element_type=jnp.float32,
    )
    for j in (2, 1, 3):
        dist_copy(j).start()
    total = dist[...]
    for j in (1, 3, 2):
        dist_copy(j).wait_recv()
        total += dists[j]
    scaled = total[0:1] * (-1.0 / math.sqrt(D))
    logit_ref[...] = jnp.where(episode_ref[...] == 0, scaled[:, 0:WAYS], scaled[:, WAYS:])

    for j in (1, 2, 3):
        dist_copy(j).wait_send()

    @pl.when(pipe == last)
    def _():
        for j in (1, 2, 3):
            sq_copy(j).wait_send()
        for j in range(1, LANES):
            part_copy(j).wait_send()
        for step in range(1, GROUPS):
            done_copy(step).wait_send()


def close(hidden, weight, gain, count, episode):
    vmem = pl.BlockSpec(memory_space=pltpu.VMEM)
    sems = pltpu.SemaphoreType.DMA
    f32 = jnp.float32
    tokens = STEPS * SLOTS
    return pl.pallas_call(
        close_kernel,
        out_shape=(
            jax.ShapeDtypeStruct((EPISODES * WAYS, SHARD), f32),
            jax.ShapeDtypeStruct((1, WAYS), f32),
        ),
        in_specs=[vmem] * 5,
        out_specs=(vmem, vmem),
        scratch_shapes=[
            pltpu.VMEM((LANES, 8, SHARD), f32),
            pltpu.VMEM((LANES, 8, SHARD), f32),
            pltpu.VMEM((8, tokens), f32),
            pltpu.VMEM((TENSOR, 8, tokens), f32),
            pltpu.VMEM((8, SHARD), f32),
            pltpu.VMEM((LANES, 8, SHARD), f32),
            pltpu.VMEM((8, EPISODES * WAYS), f32),
            pltpu.VMEM((TENSOR, 8, EPISODES * WAYS), f32),
            sems((TENSOR,)),
            sems((TENSOR,)),
            sems((LANES,)),
            sems((LANES,)),
            sems((GROUPS,)),
            sems((LANES,)),
            sems((TENSOR,)),
            sems((TENSOR,)),
        ],
        compiler_params=pltpu.CompilerParams(collective_id=2, has_side_effects=True),
        name="close",
    )(hidden, weight, gain, count, episode)


def own(table, index):
    return lax.dynamic_index_in_dim(table, index, 0, keepdims=False)


def shards(
    support_tokens,
    support_lengths,
    support_labels,
    query_tokens,
    query_lengths,
    query_episodes,
    embedding,
    attn_gain,
    query_weight,
    key_weight,
    value_weight,
    out_weight,
    final_gain,
):
    dp, pipe, tensor = place()
    mine = dp * PIPE + pipe
    table_rows = embedding.shape[0]
    row = jnp.concatenate(
        [
            support_tokens.reshape(64),
            query_tokens.reshape(32),
            support_lengths,
            query_lengths,
            support_labels.reshape(2),
            jnp.zeros((27,), jnp.int32),
        ]
    ).reshape(1, 128)
    every = share_ids(row)
    tokens = every[:, :96].reshape(96, 32)
    lengths = every[:, 96:99].reshape(96)
    labels = every[:, 99:101]
    group = jnp.arange(GROUPS)
    class_row = (labels // 4) * 8 + labels % 4
    query_row = (group // 4) * 8 + 4 + group % 4
    target = jnp.concatenate([class_row, query_row[:, None]], axis=1).reshape(96)

    index = jnp.arange(96)
    ahead = (lengths[None, :] > lengths[:, None]) | (
        (lengths[None, :] == lengths[:, None]) & (index[None, :] < index[:, None])
    )
    rank = jnp.sum(ahead.astype(jnp.int32), axis=1)
    at_rank = rank[None, :] == index[:, None]
    seq_of = jnp.sum(jnp.where(at_rank, index[None, :], 0), axis=1)
    len_of = jnp.sum(jnp.where(at_rank, lengths[None, :], 0), axis=1)
    bins = LANES * STEPS
    first_two = len_of[:bins] + len_of[bins : 2 * bins][::-1]
    bin_id = jnp.arange(bins)
    below = (first_two[None, :] < first_two[:, None]) | (
        (first_two[None, :] == first_two[:, None]) & (bin_id[None, :] < bin_id[:, None])
    )
    third = jnp.sum(below.astype(jnp.int32), axis=1)
    at_third = third[:, None] == bin_id[None, :]
    seq_third = jnp.sum(jnp.where(at_third, seq_of[None, 2 * bins :], 0), axis=1)
    len_third = jnp.sum(jnp.where(at_third, len_of[None, 2 * bins :], 0), axis=1)
    len_a, len_b, len_c = len_of[:bins], len_of[bins : 2 * bins][::-1], len_third
    seq_a, seq_b, seq_c = seq_of[:bins], seq_of[bins : 2 * bins][::-1], seq_third
    full = len_a + len_b + len_c
    slot = jnp.arange(SLOTS)[None, :]
    in_a = slot < len_a[:, None]
    in_b = slot < (len_a + len_b)[:, None]
    live = slot < full[:, None]
    seq = jnp.where(in_a, seq_a[:, None], jnp.where(in_b, seq_b[:, None], seq_c[:, None]))
    position = slot - jnp.where(
        in_a, 0, jnp.where(in_b, len_a[:, None], (len_a + len_b)[:, None])
    )
    seq_hot = (seq[:, :, None] == index[None, None, :]).astype(jnp.float32)
    facts = jnp.concatenate([tokens, lengths[:, None], target[:, None]], axis=1)
    slot_facts = jnp.dot(
        seq_hot.reshape(bins * SLOTS, 96), facts.astype(jnp.float32), precision=HIGH
    ).astype(jnp.int32)
    at_position = position.reshape(-1, 1) == jnp.arange(32)[None, :]
    token = jnp.sum(jnp.where(at_position, slot_facts[:, :32], 0), axis=1)

    count = STEPS * SLOTS
    token = token.reshape(LANES, count)
    live = live.reshape(LANES, count)
    holder = jnp.where(live, token // table_rows, GROUPS)
    local = token - holder * table_rows
    order = jnp.arange(count)
    same = (token[:, None, :] == token[:, :, None]) & live[:, None, :]
    repeated = jnp.any(same & (order[None, None, :] < order[None, :, None]), axis=2)
    leads = live & ~repeated
    before = (
        leads[:, None, :]
        & (holder[:, None, :] == holder[:, :, None])
        & (token[:, None, :] < token[:, :, None])
    )
    place_in = jnp.sum(before.astype(jnp.int32), axis=2)
    fits = jnp.all(full <= SLOTS) & jnp.all(jnp.where(live, place_in, 0) < CAP)
    wanted = (leads & (holder == mine))[:, None, :] & (
        place_in[:, None, :] == jnp.arange(CAP)[None, :, None]
    )
    picked = jnp.sum(jnp.where(wanted, local[:, None, :], 0), axis=2)

    my_live = own(live, dp)
    my_slots = jnp.where(my_live, own(holder, dp) * CAP + own(place_in, dp), -1)
    my_seq = own(seq.reshape(LANES, STEPS, SLOTS), dp)
    my_pos = own(position.reshape(LANES, STEPS, SLOTS), dp)
    my_facts = own(slot_facts.reshape(LANES, count, 34), dp)
    seen = (
        (my_seq[:, :, None] == my_seq[:, None, :])
        & (my_pos[:, None, :] <= my_pos[:, :, None])
        & my_live.reshape(STEPS, 1, SLOTS)
    )
    bias = jnp.where(seen, 0.0, -1e30).astype(jnp.float32)
    half = HEAD_DIM // 2
    freqs = jnp.exp(
        -math.log(rotary_base) * jnp.arange(half, dtype=jnp.float32) * (2.0 / HEAD_DIM)
    )
    angles = my_pos.astype(jnp.float32)[:, :, None] * freqs
    cosine, sine = jnp.cos(angles), jnp.sin(angles)
    cosine = jnp.concatenate([cosine, cosine], axis=-1)
    sine = jnp.concatenate([-sine, sine], axis=-1)
    weight = jnp.where(
        my_live[None, :] & (my_facts[:, 33][None, :] == jnp.arange(64)[:, None]),
        1.0 / my_facts[:, 32].astype(jnp.float32)[None, :],
        0.0,
    )
    own_class = dp * 4 + jnp.arange(4)
    class_count = jnp.sum(
        (labels.reshape(1, 64) == own_class[:, None]).astype(jnp.float32), axis=1
    )
    class_count = jnp.concatenate([class_count, jnp.ones((4,), jnp.float32)])[:, None]
    gain = lax.dynamic_slice_in_dim(final_gain, tensor * SHARD, SHARD).reshape(1, SHARD)
    episode = jnp.broadcast_to(query_episodes[:, None], (1, WAYS))
    rest = (
        support_tokens,
        support_lengths,
        support_labels,
        query_tokens,
        query_lengths,
        query_episodes,
        embedding,
        attn_gain,
        query_weight,
        key_weight,
        value_weight,
        out_weight,
        final_gain,
    )

    def packed(_):
        rows = jnp.take(embedding, picked.reshape(-1), axis=0).reshape(LANES, CAP, SHARD)
        hidden = trunk(
            rows,
            my_slots.reshape(STEPS, SLOTS, 1),
            cosine,
            sine,
            bias,
            attn_gain,
            query_weight,
            key_weight,
            value_weight,
            out_weight,
        )
        return close(hidden, weight, gain, class_count, episode)

    return lax.cond(fits, packed, lambda _: plain_shards(*rest), 0)


def solution(mesh):
    return jax.shard_map(
        shards,
        mesh=mesh,
        in_specs=(
            P(("dp", "pipe"), None),
            P(("dp", "pipe")),
            P(("dp", "pipe"), None),
            P(("dp", "pipe"), None),
            P(("dp", "pipe")),
            P(("dp", "pipe")),
            P(("dp", "pipe"), "tensor"),
            P("pipe", None),
            P("pipe", None, "tensor"),
            P("pipe", None, "tensor"),
            P("pipe", None, "tensor"),
            P("pipe", "tensor", None),
            P(),
        ),
        out_specs=(P(None, "tensor"), P(("dp", "pipe"), None)),
        check_vma=False,
    )
```
